32 devices in a mesh: pole: 2 (over y), prow: 4 (over z), pcol: 4 (over x, core).
Axes of the slice: x: 2, y: 2, z: 4, core: 2. Of those that a mesh axis runs over, the one named last changes fastest.
Arguments:
- ainv_anc: bfloat16 [2, 4096, 2048], P(None, ('pole', 'prow'), 'pcol'), parts along dimension 1, may hold values from -6 to 6
- panel: bfloat16 [2, 8, 1024, 256], P(None, 'pole', ('pcol', 'prow')), parts along dimension 1, may hold values from -6 to 6
- u_inv: bfloat16 [2, 8, 256, 256], P(None, 'pole'), parts along dimension 1, may hold values from -0.01171875 to 0.01171875
- k_inv: float32 [2, 8, 256, 256], P(None, ('pole', 'pcol')), parts along dimension 1, may hold values from -6 to 6
- structure: int32 [4, 4], replicated, may hold values from -1 to 7, as said below
Outputs:
- sel_inv: float32 [2, 4096, 1024], P(None, ('pole', 'prow'), 'pcol'), parts along dimension 1
- diag_inv: float32 [2, 8, 256, 256], P(None, ('pole', 'pcol')), parts along dimension 1
The draws below stay inside these ranges and needn't reach their ends.
There are 2 independent parts, one for each index of `pole`. The reference program is written for one: setup_inputs(seed, part) draws one part's arguments, and reference() takes and returns one part's arrays. A program takes and returns all parts, laid end to end along the dimension named above; an argument that names none is the same for every part. Nothing has to cross between parts.
Inputs may be any that keep to these rules, and one draw needn't show every extreme that they name: `structure`: slots g * 1 to (g + 1) * 1 - 1 of row k hold distinct blocks of g * 2 to (g + 1) * 2 - 1 in rising order, followed by -1 for empty slots; each such group of each row holds at least one block, and for every g some row fills all 1 slots of group g.
All inputs are finite; a program needn't handle non-finite values.
Results may differ from the reference program's by a relative error of at most 0.005.
Values may be sent and summed in bfloat16 or wider, within the bound.
No kernel may reach another device: no remote copies, remote signals or barrier semaphores. Data moves between devices by JAX's collectives and lax.ppermute only.
A program may use at most 128 MiB of HBM per device.

```python
import jax
import jax.numpy as jnp
from jax import lax

B = 256
NS = 8
GROUPB = 2
M = 4
GSLOT = 1
NK = 4


def draw_structure(key, part):
    groups = NS // GROUPB
    key_count = jax.random.fold_in(key, 11)
    key_full = jax.random.fold_in(key, 12)
    key_score = jax.random.fold_in(key, 13)
    counts = jax.random.randint(key_count, (NK, groups), 1, GSLOT + 1)
    full_row = jax.random.randint(key_full, (groups,), 0, NK)
    counts = jnp.where(jnp.arange(NK)[:, None] == full_row[None, :], GSLOT, counts)
    scores = jax.random.randint(key_score, (NK, groups, GROUPB), 0, 1 << 20) * GROUPB + jnp.arange(GROUPB)[None, None, :]
    order = jnp.argsort(scores, axis=-1)
    chosen = order[:, :, :GSLOT]
    slot_index = jnp.arange(GSLOT)
    live_slot = slot_index[None, None, :] < counts[:, :, None]
    keyed = jnp.where(live_slot, chosen, GROUPB + slot_index[None, None, :])
    ranked = jnp.sort(keyed, axis=-1)
    offset = jnp.arange(groups)[None, :, None] * GROUPB
    result = jnp.where(ranked < GROUPB, ranked + offset, -1)
    return result.reshape(NK, groups * GSLOT).astype(jnp.int32)


def block_levels(key, shape, cuts, least, high):
    gain = 1.0
    for position, parts in cuts:
        steps = jax.random.uniform(jax.random.fold_in(jax.random.fold_in(key, 6), position), (parts,), jnp.float32, least / len(cuts), high / len(cuts))
        gain = gain * jnp.repeat(jnp.exp(steps), shape[position] // parts).reshape((-1,) + (1,) * (len(shape) - 1 - position))
    return gain


def noise(stream_key, shape, deviation, reach, pieces=(), kind=jnp.bfloat16):
    gain = block_levels(stream_key, shape, pieces, -0.22, 0.18) if pieces else 1.0
    values = jax.random.normal(stream_key, shape, jnp.float32) * deviation * gain
    return jnp.minimum(jnp.maximum(values, -reach), reach).astype(kind)


def setup_inputs(seed: int = 0, part: int = 0) -> dict:
    splits = jax.random.split(jax.random.key(seed), 6)
    part_splits = jax.random.split(jax.random.fold_in(splits[5], part), 6)
    return {
        "ainv_anc": noise(part_splits[0], (2, NS * B, NS * B), 1.0, 6.0, ((1, 4), (2, 4))),
        "panel": noise(part_splits[1], (2, NK, M * B, B), 1.0, 6.0, ((2, 16),)),
        "u_inv": noise(part_splits[2], (2, NK, B, B), (B * B * M) ** -0.5, 0.01171875),
        "k_inv": noise(part_splits[3], (2, NK, B, B), 1.0, 6.0, ((1, 4),), jnp.float32),
        "structure": draw_structure(jax.random.fold_in(splits[5], 71), part),
    }


def complex_dot(left, right):
    real = jnp.dot(left[0], right[0], preferred_element_type=jnp.float32) - jnp.dot(left[1], right[1], preferred_element_type=jnp.float32)
    imag = jnp.dot(left[0], right[1], preferred_element_type=jnp.float32) + jnp.dot(left[1], right[0], preferred_element_type=jnp.float32)
    return jnp.stack([real, imag])


def complex_tdot(left, right):
    highest = lax.Precision.HIGHEST
    real = jnp.dot(left[0].T, right[0], precision=highest) - jnp.dot(left[1].T, right[1], precision=highest)
    imag = jnp.dot(left[0].T, right[1], precision=highest) + jnp.dot(left[1].T, right[0], precision=highest)
    return jnp.stack([real, imag])


def reference(ainv_anc, panel, u_inv, k_inv, structure):
    highest = lax.Precision.HIGHEST
    blocks = ainv_anc.reshape(2, NS, B, NS, B)

    def one_node(items):
        panel_k, slot_ids, u_block, k_block = items
        live_slots = slot_ids >= 0
        safe_ids = jnp.where(live_slots, slot_ids, 0).astype(jnp.int32)
        live_rows = jnp.repeat(live_slots, B)
        scaled = complex_dot(panel_k, u_block)
        scaled = jnp.where(live_rows[None, :, None], scaled, 0.0).astype(jnp.bfloat16)
        picked = jnp.take(jnp.take(blocks, safe_ids, axis=1), safe_ids, axis=3).reshape(2, M * B, M * B)
        result = -complex_dot(picked, scaled)
        result = jnp.where(live_rows[None, :, None], result, 0.0)
        diag_k = k_block - complex_tdot(scaled.astype(jnp.float32), result)
        onehot = (slot_ids[:, None] == jnp.arange(NS, dtype=jnp.int32)[None, :]).astype(jnp.float32)
        dense = jnp.einsum("mj,cmab->cjab", onehot, result.reshape(2, M, B, B), precision=highest)
        return dense, diag_k

    items = (jnp.moveaxis(panel, 1, 0), structure, jnp.moveaxis(u_inv, 1, 0), jnp.moveaxis(k_inv, 1, 0))
    dense, diag_inv = lax.map(one_node, items)
    sel_inv = jnp.transpose(dense, (1, 2, 3, 0, 4)).reshape(2, NS * B, NK * B)
    return sel_inv, jnp.moveaxis(diag_inv, 0, 1)
```

```python
import jax
import jax.numpy as jnp
from jax import lax
from jax.experimental import pallas as pl
from jax.experimental.pallas import tpu as pltpu
from jax.sharding import PartitionSpec as P

BF16 = jnp.bfloat16
F32 = jnp.float32
ANY = pl.BlockSpec(memory_space=pl.ANY)
VMEM = pl.BlockSpec(memory_space=pltpu.VMEM)
SMEM = pl.BlockSpec(memory_space=pltpu.SMEM)


def swap(x, axis, d):
    n = lax.axis_size(axis)
    return lax.ppermute(x, axis, [(i, i ^ d) for i in range(n)])


def run_copies(copies):
    for copy in copies:
        copy.start()
    for copy in copies:
        copy.wait()


def pick_panel(panel, own_k):
    n_cols = lax.axis_size("pcol")
    planes, _, rows, width = panel.shape

    def kernel(panel_ref, *refs):
        outs, sems = refs[:n_cols], refs[n_cols]
        col = lax.axis_index("pcol")
        run_copies(
            [
                pltpu.make_async_copy(
                    panel_ref.at[:, pl.ds((col ^ d) * own_k, own_k)], outs[d], sems.at[d]
                )
                for d in range(n_cols)
            ]
        )

    return pl.pallas_call(
        kernel,
        name="pick_panel",
        in_specs=[ANY],
        out_specs=[ANY] * n_cols,
        out_shape=[jax.ShapeDtypeStruct((planes, own_k, rows, width), panel.dtype)] * n_cols,
        scratch_shapes=[pltpu.SemaphoreType.DMA((n_cols,))],
    )(panel)


class Rows:
    def __init__(self, row_blocks, group_blocks, group_slots):
        self.row_blocks, self.group_blocks, self.group_slots = row_blocks, group_blocks, group_slots
        nested = row_blocks % group_blocks == 0 or group_blocks % row_blocks == 0
        slots = max(row_blocks // group_blocks, 1) * group_slots
        self.by_slot = nested and slots < row_blocks
        self.count = slots if self.by_slot else row_blocks

    def entry(self, struct_ref, node, row, index):
        base = row * self.row_blocks
        if self.by_slot:
            slot = (base // self.group_blocks) * self.group_slots + index
            block = struct_ref[node, slot] - base
            live = jnp.logical_and(block >= 0, block < self.row_blocks)
            return jnp.where(live, block, 0), live, slot // self.group_slots, slot % self.group_slots
        target = base + index
        group = target // self.group_blocks
        found, live = jnp.int32(0), jnp.int32(0)
        for s in range(self.group_slots):
            hit = struct_ref[node, group * self.group_slots + s] == target
            found = jnp.where(hit, s, found)
            live = jnp.where(hit, 1, live)
        return jnp.int32(index), live > 0, group, found


def pick_ainv(ainv, u_inv, structure, own_k, rows):
    n_cols = lax.axis_size("pcol")
    width = u_inv.shape[-1]
    slots = rows.group_slots

    def kernel(struct_ref, ainv_ref, u_ref, *refs):
        outs, u_out, sems, u_sem = refs[:n_cols], refs[n_cols], refs[n_cols + 1], refs[n_cols + 2]
        col, row = lax.axis_index("pcol"), lax.axis_index("prow")
        copies = [pltpu.make_async_copy(u_ref.at[:, pl.ds(col * own_k, own_k)], u_out, u_sem)]
        for d in range(n_cols):
            for kk in range(own_k):
                node = (col ^ d) * own_k + kk
                for i in range(rows.count):
                    block, _, _, _ = rows.entry(struct_ref, node, row, i)
                    for s in range(slots):
                        j = struct_ref[node, col * slots + s] - col * rows.group_blocks
                        j = jnp.maximum(j, 0)
                        copies.append(
                            pltpu.make_async_copy(
                                ainv_ref.at[:, pl.ds(block * width, width), pl.ds(j * width, width)],
                                outs[d].at[:, kk, pl.ds(i * width, width), pl.ds(s * width, width)],
                                sems.at[d, kk, i, s],
                            )
                        )
        run_copies(copies)

    shape = jax.ShapeDtypeStruct((2, own_k, rows.count * width, slots * width), ainv.dtype)
    out = pl.pallas_call(
        kernel,
        name="pick_ainv",
        in_specs=[SMEM, ANY, ANY],
        out_specs=[ANY] * (n_cols + 1),
        out_shape=[shape] * n_cols + [jax.ShapeDtypeStruct((2, own_k, width, width), u_inv.dtype)],
        scratch_shapes=[
            pltpu.SemaphoreType.DMA((n_cols, own_k, rows.count, slots)),
            pltpu.SemaphoreType.DMA,
        ],
    )(structure, ainv, u_inv)
    return out[:n_cols], out[n_cols]


def dot(left, right):
    return jnp.dot(left, right, preferred_element_type=F32)


def tdot(left, right):
    return lax.dot_general(left, right, (((0,), (0,)), ((), ())), preferred_element_type=F32)


def solve(structure, own, rest, ainv, u_own, rows):
    n_rows, n_cols = lax.axis_size("prow"), lax.axis_size("pcol")
    _, own_k, part, width = own[0].shape
    slots = rows.group_slots
    sub = min(part, width)
    band = width // n_rows

    def kernel(struct_ref, u_ref, *refs):
        own_refs, refs = refs[:n_rows], refs[n_rows:]
        rest_refs, refs = refs[:n_rows], refs[n_rows:]
        ainv_refs, refs = refs[:n_cols], refs[n_cols:]
        sel_ref, q_refs, (scaled, quad) = refs[0], refs[1 : 1 + n_rows], refs[1 + n_rows :]
        col, row = lax.axis_index("pcol"), lax.axis_index("prow")
        if rows.by_slot:
            sel_ref[...] = jnp.zeros_like(sel_ref)
        for kk in range(own_k):
            node = col * own_k + kk
            u_real, u_imag = u_ref[0, kk], u_ref[1, kk]
            for dz in range(n_rows):
                first = (row ^ dz) * part
                for real, imag, dxs in (
                    (own_refs[dz][0, kk], own_refs[dz][1, kk], (0,)),
                    (
                        rest_refs[dz][:, 0, kk].reshape((n_cols - 1) * part, width),
                        rest_refs[dz][:, 1, kk].reshape((n_cols - 1) * part, width),
                        tuple(range(1, n_cols)),
                    ),
                ):
                    s_real = dot(real, u_real) - dot(imag, u_imag)
                    s_imag = dot(real, u_imag) + dot(imag, u_real)
                    for n, dx in enumerate(dxs):
                        for o in range(0, part, sub):
                            slot = (first + o) // width
                            live = struct_ref[node, (col ^ dx) * slots + slot] >= 0
                            at = pl.ds(pl.multiple_of(first + o, sub), sub)
                            for plane, value in ((0, s_real), (1, s_imag)):
                                piece = value[n * part + o : n * part + o + sub]
                                scaled[plane, kk, dx, at, :] = jnp.where(live, piece, 0.0).astype(BF16)
            q_real = jnp.zeros((width, width), F32)
            q_imag = jnp.zeros((width, width), F32)
            for i in range(rows.count):
                block, live, group, slot = rows.entry(struct_ref, node, row, i)
                here = slice(i * width, (i + 1) * width)
                acc_real = jnp.zeros((width, width), F32)
                acc_imag = jnp.zeros((width, width), F32)
                for dx in range(n_cols):
                    a_real, a_imag = ainv_refs[dx][0, kk, here, :], ainv_refs[dx][1, kk, here, :]
                    s_real, s_imag = scaled[0, kk, dx], scaled[1, kk, dx]
                    acc_real += dot(a_real, s_real) - dot(a_imag, s_imag)
                    acc_imag += dot(a_real, s_imag) + dot(a_imag, s_real)
                sel_real = jnp.where(live, -acc_real, 0.0)
                sel_imag = jnp.where(live, -acc_imag, 0.0)

                def put(block=block, sel_real=sel_real, sel_imag=sel_imag, kk=kk):
                    at = pl.ds(pl.multiple_of(block * width, width), width)
                    sel_ref[0, at, kk * width : (kk + 1) * width] = sel_real
                    sel_ref[1, at, kk * width : (kk + 1) * width] = sel_imag

                if rows.by_slot:
                    pl.when(live)(put)
                else:
                    put()
                at = pl.ds(pl.multiple_of(slot * width, width), width)
                left_real, left_imag = scaled[0, kk, group ^ col, at, :], scaled[1, kk, group ^ col, at, :]
                hi_real, hi_imag = sel_real.astype(BF16), sel_imag.astype(BF16)
                lo_real = (sel_real - hi_real.astype(F32)).astype(BF16)
                lo_imag = (sel_imag - hi_imag.astype(F32)).astype(BF16)
                right = jnp.concatenate([hi_real, hi_imag, lo_real, lo_imag], axis=1)
                by_real, by_imag = tdot(left_real, right), tdot(left_imag, right)
                by_real = by_real[:, : 2 * width] + by_real[:, 2 * width :]
                by_imag = by_imag[:, : 2 * width] + by_imag[:, 2 * width :]
                q_real += by_real[:, :width] - by_imag[:, width:]
                q_imag += by_real[:, width:] + by_imag[:, :width]
            quad[0], quad[1] = q_real, q_imag
            for dz in range(n_rows):
                at = pl.ds(pl.multiple_of((row ^ dz) * band, band), band)
                for plane in range(2):
                    q_refs[dz][plane, kk] = quad[plane, at, :].astype(q_refs[dz].dtype)

    chunk = (2, own_k, band, width)
    out = pl.pallas_call(
        kernel,
        name="solve",
        in_specs=[SMEM] + [VMEM] * (1 + 2 * n_rows + n_cols),
        out_specs=[VMEM] * (1 + n_rows),
        out_shape=[
            jax.ShapeDtypeStruct((2, rows.row_blocks * width, own_k * width), F32),
            jax.ShapeDtypeStruct(chunk, F32),
        ]
        + [jax.ShapeDtypeStruct(chunk, BF16)] * (n_rows - 1),
        scratch_shapes=[
            pltpu.VMEM((2, own_k, n_cols, slots * width, width), BF16),
            pltpu.VMEM((2, width, width), F32),
        ],
    )(structure, u_own, *own, *rest, *ainv)
    return out[0], out[1:]


def finish_band(k_inv, terms):
    def kernel(k_ref, *refs):
        *term_refs, out_ref = refs
        row = lax.axis_index("prow")
        band = out_ref.shape[2]
        total = term_refs[0][...]
        for ref in term_refs[1:]:
            total += ref[...].astype(F32)
        at = pl.ds(pl.multiple_of(row * band, band), band)
        out_ref[...] = (k_ref[:, :, at, :] - total).astype(BF16)

    return pl.pallas_call(
        kernel,
        name="finish_band",
        in_specs=[VMEM] * (1 + len(terms)),
        out_specs=VMEM,
        out_shape=jax.ShapeDtypeStruct(terms[0].shape, BF16),
    )(k_inv, *terms)


def join_bands(bands, shape):
    def kernel(*refs):
        *band_refs, out_ref = refs
        row = lax.axis_index("prow")
        band = band_refs[0].shape[2]
        for d, ref in enumerate(band_refs):
            at = pl.ds(pl.multiple_of((row ^ d) * band, band), band)
            out_ref[:, :, at, :] = ref[...].astype(F32)

    return pl.pallas_call(
        kernel,
        name="join_bands",
        in_specs=[VMEM] * len(bands),
        out_specs=VMEM,
        out_shape=jax.ShapeDtypeStruct(shape, F32),
    )(*bands)


def gather_rows(x):
    n = lax.axis_size("prow")
    held = {0: x}
    d = n // 2
    while d:
        held.update({at ^ d: swap(value, "prow", d) for at, value in list(held.items())})
        d //= 2
    return [held[d] for d in range(n)]


def local(ainv_anc, panel, u_inv, k_inv, structure):
    width = u_inv.shape[-1]
    own_k = k_inv.shape[1]
    n_rows, n_cols = lax.axis_size("prow"), lax.axis_size("pcol")
    rows = Rows(ainv_anc.shape[1] // width, ainv_anc.shape[2] // width, structure.shape[1] // n_cols)
    parts = pick_panel(panel, own_k)
    own = gather_rows(parts[0])
    got = [swap(parts[d], "pcol", d) for d in range(1, n_cols)]
    rest = gather_rows(jnp.stack(got))
    blocks, u_own = pick_ainv(ainv_anc, u_inv, structure, own_k, rows)
    ainv = [blocks[0]] + [swap(blocks[d], "pcol", d) for d in range(1, n_cols)]
    sel_inv, terms = solve(structure, own, rest, ainv, u_own, rows)
    terms = [terms[0]] + [swap(terms[d], "prow", d) for d in range(1, n_rows)]
    mine = finish_band(k_inv, terms)
    bands = [mine] + [swap(mine, "prow", d) for d in range(1, n_rows)]
    return sel_inv, join_bands(bands, k_inv.shape)


def solution(mesh):
    placed = (
        P(None, ("pole", "prow"), "pcol"),
        P(None, "pole", ("pcol", "prow"), None),
        P(None, "pole", None, None),
        P(None, ("pole", "pcol"), None, None),
        P(),
    )
    return jax.shard_map(
        local,
        mesh=mesh,
        in_specs=placed,
        out_specs=(P(None, ("pole", "prow"), "pcol"), P(None, ("pole", "pcol"), None, None)),
        check_vma=False,
    )
```

```python
import jax
import jax.numpy as jnp
from jax import lax
from jax.experimental import pallas as pl
from jax.experimental.pallas import tpu as pltpu
from jax.sharding import PartitionSpec as P

BF16 = jnp.bfloat16
F32 = jnp.float32
FEW = 8
ANY = pl.BlockSpec(memory_space=pl.ANY)
HBM = pl.BlockSpec(memory_space=pltpu.HBM)
VMEM = pl.BlockSpec(memory_space=pltpu.VMEM)
SMEM = pl.BlockSpec(memory_space=pltpu.SMEM)


def swap(x, axis, d):
    n = lax.axis_size(axis)
    return lax.ppermute(x, axis, [(i, i ^ d) for i in range(n)])


def nbytes(*arrays):
    return sum(a.size * a.dtype.itemsize for a in arrays)


def limits(*arrays):
    return pltpu.CompilerParams(vmem_limit_bytes=nbytes(*arrays) + (4 << 20))


def run_copies(copies):
    for copy in copies:
        copy.start()
    for copy in copies:
        copy.wait()


def pick_panel(panel, own_k):
    n_cols = lax.axis_size("pcol")
    planes, _, rows, width = panel.shape

    def kernel(panel_ref, *refs):
        outs, sems = refs[:n_cols], refs[n_cols]
        col = lax.axis_index("pcol")
        run_copies(
            [
                pltpu.make_async_copy(
                    panel_ref.at[:, pl.ds((col ^ d) * own_k, own_k)], outs[d], sems.at[d]
                )
                for d in range(n_cols)
            ]
        )

    outs = [jax.ShapeDtypeStruct((planes, own_k, rows, width), panel.dtype)] * n_cols
    return pl.pallas_call(
        kernel,
        name="pick_panel",
        in_specs=[HBM],
        out_specs=[VMEM] * n_cols,
        out_shape=outs,
        scratch_shapes=[pltpu.SemaphoreType.DMA((n_cols,))],
        compiler_params=limits(*outs),
    )(panel)


class Rows:
    def __init__(self, row_blocks, group_blocks, group_slots):
        self.row_blocks, self.group_blocks, self.group_slots = row_blocks, group_blocks, group_slots
        nested = row_blocks % group_blocks == 0 or group_blocks % row_blocks == 0
        slots = max(row_blocks // group_blocks, 1) * group_slots
        self.by_slot = nested and slots < row_blocks
        self.count = slots if self.by_slot else row_blocks

    def entry(self, struct_ref, node, row, index):
        base = row * self.row_blocks
        if self.by_slot:
            slot = (base // self.group_blocks) * self.group_slots + index
            block = struct_ref[node, slot] - base
            live = jnp.logical_and(block >= 0, block < self.row_blocks)
            return jnp.where(live, block, 0), live, slot // self.group_slots, slot % self.group_slots
        target = base + index
        group = target // self.group_blocks
        found, live = jnp.int32(0), jnp.int32(0)
        for s in range(self.group_slots):
            hit = struct_ref[node, group * self.group_slots + s] == target
            found = jnp.where(hit, s, found)
            live = jnp.where(hit, 1, live)
        return jnp.int32(index), live > 0, group, found


def pick_ainv(ainv, u_inv, structure, own_k, rows):
    n_cols = lax.axis_size("pcol")
    width = u_inv.shape[-1]
    slots = rows.group_slots

    def kernel(struct_ref, ainv_ref, u_ref, *refs):
        outs, u_out, sems, u_sem = refs[:n_cols], refs[n_cols], refs[n_cols + 1], refs[n_cols + 2]
        col, row = lax.axis_index("pcol"), lax.axis_index("prow")
        copies = [pltpu.make_async_copy(u_ref.at[:, pl.ds(col * own_k, own_k)], u_out, u_sem)]
        for d in range(n_cols):
            for kk in range(own_k):
                node = (col ^ d) * own_k + kk
                for i in range(rows.count):
                    block, _, _, _ = rows.entry(struct_ref, node, row, i)
                    for s in range(slots):
                        j = struct_ref[node, col * slots + s] - col * rows.group_blocks
                        j = jnp.maximum(j, 0)
                        copies.append(
                            pltpu.make_async_copy(
                                ainv_ref.at[:, pl.ds(block * width, width), pl.ds(j * width, width)],
                                outs[d].at[:, kk, pl.ds(i * width, width), pl.ds(s * width, width)],
                                sems.at[d, kk, i, s],
                            )
                        )
        run_copies(copies)

    shape = jax.ShapeDtypeStruct((2, own_k, rows.count * width, slots * width), ainv.dtype)
    outs = [shape] * n_cols + [jax.ShapeDtypeStruct((2, own_k, width, width), u_inv.dtype)]
    out = pl.pallas_call(
        kernel,
        name="pick_ainv",
        in_specs=[SMEM, ANY, ANY],
        out_specs=[VMEM] * (n_cols + 1),
        out_shape=outs,
        compiler_params=limits(*outs),
        scratch_shapes=[
            pltpu.SemaphoreType.DMA((n_cols, own_k, rows.count, slots)),
            pltpu.SemaphoreType.DMA,
        ],
    )(structure, ainv, u_inv)
    return out[:n_cols], out[n_cols]


def dot(left, right):
    return jnp.dot(left, right, preferred_element_type=F32)


def tdot(left, right):
    return lax.dot_general(left, right, (((0,), (0,)), ((), ())), preferred_element_type=F32)


def solve(structure, own, rest, ainv, u_own, rows):
    n_rows, n_cols = lax.axis_size("prow"), lax.axis_size("pcol")
    _, own_k, part, width = own[0].shape[-4:]
    few = len(own) == n_rows
    slots = rows.group_slots
    sub = min(part, width)
    band = width // n_rows

    def kernel(struct_ref, u_ref, *refs):
        own_refs, refs = refs[: len(own)], refs[len(own) :]
        rest_refs, refs = refs[: len(rest)], refs[len(rest) :]
        ainv_refs, refs = refs[:n_cols], refs[n_cols:]
        sel_ref, *q_refs, scaled, quad = refs
        col, row = lax.axis_index("pcol"), lax.axis_index("prow")
        if rows.by_slot:
            sel_ref[...] = jnp.zeros_like(sel_ref)
        for kk in range(own_k):
            node = col * own_k + kk
            u_real, u_imag = u_ref[0, kk], u_ref[1, kk]

            def scale(own_ref, rest_ref, member, node=node, kk=kk, u_real=u_real, u_imag=u_imag):
                first = member * part
                for real, imag, dxs in (
                    (own_ref[0, kk], own_ref[1, kk], (0,)),
                    (
                        rest_ref[:, 0, kk].reshape((n_cols - 1) * part, width),
                        rest_ref[:, 1, kk].reshape((n_cols - 1) * part, width),
                        tuple(range(1, n_cols)),
                    ),
                ):
                    s_real = dot(real, u_real) - dot(imag, u_imag)
                    s_imag = dot(real, u_imag) + dot(imag, u_real)
                    for n, dx in enumerate(dxs):
                        for o in range(0, part, sub):
                            slot = (first + o) // width
                            live = struct_ref[node, (col ^ dx) * slots + slot] >= 0
                            at = pl.ds(pl.multiple_of(first + o, sub), sub)
                            for plane, value in ((0, s_real), (1, s_imag)):
                                piece = value[n * part + o : n * part + o + sub]
                                scaled[plane, kk, dx, at, :] = jnp.where(live, piece, 0.0).astype(BF16)

            if few:
                for dz in range(n_rows):
                    scale(own_refs[dz], rest_refs[dz], row ^ dz)
            else:

                @pl.loop(0, n_rows)
                def _(i, scale=scale):
                    scale(own_refs[0].at[i], rest_refs[0].at[i], i)

            q_real = jnp.zeros((width, width), F32)
            q_imag = jnp.zeros((width, width), F32)
            for i in range(rows.count):
                block, live, group, slot = rows.entry(struct_ref, node, row, i)
                here = slice(i * width, (i + 1) * width)
                acc_real = jnp.zeros((width, width), F32)
                acc_imag = jnp.zeros((width, width), F32)
                for dx in range(n_cols):
                    a_real, a_imag = ainv_refs[dx][0, kk, here, :], ainv_refs[dx][1, kk, here, :]
                    s_real, s_imag = scaled[0, kk, dx], scaled[1, kk, dx]
                    acc_real += dot(a_real, s_real) - dot(a_imag, s_imag)
                    acc_imag += dot(a_real, s_imag) + dot(a_imag, s_real)
                sel_real = jnp.where(live, -acc_real, 0.0)
                sel_imag = jnp.where(live, -acc_imag, 0.0)

                def put(block=block, sel_real=sel_real, sel_imag=sel_imag, kk=kk):
                    at = pl.ds(pl.multiple_of(block * width, width), width)
                    sel_ref[0, at, kk * width : (kk + 1) * width] = sel_real
                    sel_ref[1, at, kk * width : (kk + 1) * width] = sel_imag

                if rows.by_slot:
                    pl.when(live)(put)
                else:
                    put()
                at = pl.ds(pl.multiple_of(slot * width, width), width)
                left_real, left_imag = scaled[0, kk, group ^ col, at, :], scaled[1, kk, group ^ col, at, :]
                hi_real, hi_imag = sel_real.astype(BF16), sel_imag.astype(BF16)
                lo_real = (sel_real - hi_real.astype(F32)).astype(BF16)
                lo_imag = (sel_imag - hi_imag.astype(F32)).astype(BF16)
                right = jnp.concatenate([hi_real, hi_imag, lo_real, lo_imag], axis=1)
                by_real, by_imag = tdot(left_real, right), tdot(left_imag, right)
                by_real = by_real[:, : 2 * width] + by_real[:, 2 * width :]
                by_imag = by_imag[:, : 2 * width] + by_imag[:, 2 * width :]
                q_real += by_real[:, :width] - by_imag[:, width:]
                q_imag += by_real[:, width:] + by_imag[:, :width]
            quad[0], quad[1] = q_real, q_imag
            if few:
                for dz in range(n_rows):
                    at = pl.ds(pl.multiple_of((row ^ dz) * band, band), band)
                    for plane in range(2):
                        q_refs[dz][plane, kk] = quad[plane, at, :].astype(q_refs[dz].dtype)
            else:
                for plane in range(2):
                    q_refs[0][plane, kk] = quad[plane].astype(BF16)

    sel = jax.ShapeDtypeStruct((2, rows.row_blocks * width, own_k * width), F32)
    chunk = (2, own_k, band, width)
    if few:
        terms = [jax.ShapeDtypeStruct(chunk, F32)] + [jax.ShapeDtypeStruct(chunk, BF16)] * (n_rows - 1)
    else:
        terms = [jax.ShapeDtypeStruct((2, own_k, width, width), BF16)]
    scaled = jax.ShapeDtypeStruct((2, own_k, n_cols, slots * width, width), BF16)
    quad = jax.ShapeDtypeStruct((2, width, width), F32)
    out = pl.pallas_call(
        kernel,
        name="solve",
        in_specs=[SMEM] + [VMEM] * (1 + len(own) + len(rest) + n_cols),
        out_specs=[VMEM] * (1 + len(terms)),
        out_shape=[sel] + terms,
        scratch_shapes=[pltpu.VMEM(scaled.shape, scaled.dtype), pltpu.VMEM(quad.shape, quad.dtype)],
        compiler_params=limits(sel, *terms, scaled, quad, u_own, *own, *rest, *ainv),
    )(structure, u_own, *own, *rest, *ainv)
    return out[0], out[1:]


def finish_band(k_inv, terms):
    def kernel(k_ref, *refs):
        *term_refs, out_ref = refs
        row = lax.axis_index("prow")
        band = out_ref.shape[2]
        total = term_refs[0][...].astype(F32)
        for ref in term_refs[1:]:
            total += ref[...].astype(F32)
        at = pl.ds(pl.multiple_of(row * band, band), band)
        out_ref[...] = (k_ref[:, :, at, :] - total).astype(BF16)

    return pl.pallas_call(
        kernel,
        name="finish_band",
        in_specs=[VMEM] * (1 + len(terms)),
        out_specs=VMEM,
        out_shape=jax.ShapeDtypeStruct(terms[0].shape, BF16),
        compiler_params=limits(k_inv, *terms),
    )(k_inv, *terms)


def join_bands(bands, shape):
    def kernel(*refs):
        *band_refs, out_ref = refs
        row = lax.axis_index("prow")
        band = band_refs[0].shape[2]
        for d, ref in enumerate(band_refs):
            at = pl.ds(pl.multiple_of((row ^ d) * band, band), band)
            out_ref[:, :, at, :] = ref[...].astype(F32)

    return pl.pallas_call(
        kernel,
        name="join_bands",
        in_specs=[VMEM] * len(bands),
        out_specs=VMEM,
        out_shape=jax.ShapeDtypeStruct(shape, F32),
        compiler_params=limits(jax.ShapeDtypeStruct(shape, F32), *bands),
    )(*bands)


def gather_rows(x):
    n = lax.axis_size("prow")
    if n > FEW:
        return [lax.all_gather(x, "prow")]
    held = {0: x}
    d = n // 2
    while d:
        held.update({at ^ d: swap(value, "prow", d) for at, value in list(held.items())})
        d //= 2
    return [held[d] for d in range(n)]


def local(ainv_anc, panel, u_inv, k_inv, structure):
    width = u_inv.shape[-1]
    own_k = k_inv.shape[1]
    n_rows, n_cols = lax.axis_size("prow"), lax.axis_size("pcol")
    rows = Rows(ainv_anc.shape[1] // width, ainv_anc.shape[2] // width, structure.shape[1] // n_cols)
    parts = pick_panel(panel, own_k)
    own = gather_rows(parts[0])
    got = [swap(parts[d], "pcol", d) for d in range(1, n_cols)]
    rest = gather_rows(jnp.stack(got))
    blocks, u_own = pick_ainv(ainv_anc, u_inv, structure, own_k, rows)
    ainv = [blocks[0]] + [swap(blocks[d], "pcol", d) for d in range(1, n_cols)]
    sel_inv, terms = solve(structure, own, rest, ainv, u_own, rows)
    if n_rows > FEW:
        total = lax.psum_scatter(terms[0], "prow", scatter_dimension=2, tiled=True)
        mine = finish_band(k_inv, [total])
        return sel_inv, lax.all_gather(mine, "prow", axis=2, tiled=True).astype(F32)
    terms = [terms[0]] + [swap(terms[d], "prow", d) for d in range(1, n_rows)]
    mine = finish_band(k_inv, terms)
    bands = [mine] + [swap(mine, "prow", d) for d in range(1, n_rows)]
    return sel_inv, join_bands(bands, k_inv.shape)


def solution(mesh):
    placed = (
        P(None, ("pole", "prow"), "pcol"),
        P(None, "pole", ("pcol", "prow"), None),
        P(None, "pole", None, None),
        P(None, ("pole", "pcol"), None, None),
        P(),
    )
    return jax.shard_map(
        local,
        mesh=mesh,
        in_specs=placed,
        out_specs=(P(None, ("pole", "prow"), "pcol"), P(None, ("pole", "pcol"), None, None)),
        check_vma=False,
    )
```

```python
import jax
import jax.numpy as jnp
from jax import lax
from jax.experimental import pallas as pl
from jax.experimental.pallas import tpu as pltpu
from jax.sharding import PartitionSpec as P

BF16 = jnp.bfloat16
F32 = jnp.float32
FEW = 8
ANY = pl.BlockSpec(memory_space=pl.ANY)
HBM = pl.BlockSpec(memory_space=pltpu.HBM)
VMEM = pl.BlockSpec(memory_space=pltpu.VMEM)
SMEM = pl.BlockSpec(memory_space=pltpu.SMEM)


def swap(x, axis, d):
    n = lax.axis_size(axis)
    return lax.ppermute(x, axis, [(i, i ^ d) for i in range(n)])


def nbytes(*arrays):
    return sum(a.size * a.dtype.itemsize for a in arrays)


def limits(*arrays):
    return pltpu.CompilerParams(vmem_limit_bytes=nbytes(*arrays) + (4 << 20))


def run_copies(copies):
    for copy in copies:
        copy.start()
    for copy in copies:
        copy.wait()


def pick_panel(panel, own_k):
    n_cols = lax.axis_size("pcol")
    planes, _, rows, width = panel.shape

    def kernel(panel_ref, *refs):
        outs, sems = refs[:n_cols], refs[n_cols]
        col = lax.axis_index("pcol")
        run_copies(
            [
                pltpu.make_async_copy(
                    panel_ref.at[:, pl.ds((col ^ d) * own_k, own_k)], outs[d], sems.at[d]
                )
                for d in range(n_cols)
            ]
        )

    outs = [jax.ShapeDtypeStruct((planes, own_k, rows, width), panel.dtype)] * n_cols
    return pl.pallas_call(
        kernel,
        name="pick_panel",
        in_specs=[HBM],
        out_specs=[VMEM] * n_cols,
        out_shape=outs,
        scratch_shapes=[pltpu.SemaphoreType.DMA((n_cols,))],
        compiler_params=limits(*outs),
    )(panel)


class Rows:
    def __init__(self, row_blocks, group_blocks, group_slots):
        self.row_blocks, self.group_blocks, self.group_slots = row_blocks, group_blocks, group_slots
        nested = row_blocks % group_blocks == 0 or group_blocks % row_blocks == 0
        slots = max(row_blocks // group_blocks, 1) * group_slots
        self.by_slot = nested and slots < row_blocks
        self.count = slots if self.by_slot else row_blocks

    def entry(self, struct_ref, node, row, index):
        base = row * self.row_blocks
        if self.by_slot:
            slot = (base // self.group_blocks) * self.group_slots + index
            block = struct_ref[node, slot] - base
            live = jnp.logical_and(block >= 0, block < self.row_blocks)
            return jnp.where(live, block, 0), live, slot // self.group_slots, slot % self.group_slots
        target = base + index
        group = target // self.group_blocks
        found, live = jnp.int32(0), jnp.int32(0)
        for s in range(self.group_slots):
            hit = struct_ref[node, group * self.group_slots + s] == target
            found = jnp.where(hit, s, found)
            live = jnp.where(hit, 1, live)
        return jnp.int32(index), live > 0, group, found


def pick_ainv(ainv, structure, own_k, width, rows):
    n_cols = lax.axis_size("pcol")
    slots = rows.group_slots

    def kernel(struct_ref, ainv_ref, *refs):
        outs, sems = refs[:n_cols], refs[n_cols]
        col, row = lax.axis_index("pcol"), lax.axis_index("prow")
        copies = []
        for d in range(n_cols):
            for kk in range(own_k):
                node = (col ^ d) * own_k + kk
                for i in range(rows.count):
                    block, _, _, _ = rows.entry(struct_ref, node, row, i)
                    for s in range(slots):
                        j = struct_ref[node, col * slots + s] - col * rows.group_blocks
                        j = jnp.maximum(j, 0)
                        copies.append(
                            pltpu.make_async_copy(
                                ainv_ref.at[:, pl.ds(block * width, width), pl.ds(j * width, width)],
                                outs[d].at[:, kk, pl.ds(i * width, width), pl.ds(s * width, width)],
                                sems.at[d, kk, i, s],
                            )
                        )
        run_copies(copies)

    shape = jax.ShapeDtypeStruct((2, own_k, rows.count * width, slots * width), ainv.dtype)
    return pl.pallas_call(
        kernel,
        name="pick_ainv",
        in_specs=[SMEM, ANY],
        out_specs=[VMEM] * n_cols,
        out_shape=[shape] * n_cols,
        scratch_shapes=[pltpu.SemaphoreType.DMA((n_cols, own_k, rows.count, slots))],
        compiler_params=limits(*[shape] * n_cols),
    )(structure, ainv)


def dot(left, right):
    return jnp.dot(left, right, preferred_element_type=F32)


def tdot(left, right):
    return lax.dot_general(left, right, (((0,), (0,)), ((), ())), preferred_element_type=F32)


def scale(struct_ref, u_ref, ref, dxs, member, out, at_dx):
    n_cols = lax.axis_size("pcol")
    col = lax.axis_index("pcol")
    _, _, own_k, part, width = ref.shape
    slots = struct_ref.shape[1] // n_cols
    sub = min(part, width)
    first = member * part
    for kk in range(own_k):
        node = col * own_k + kk
        u_real, u_imag = u_ref[0, node], u_ref[1, node]
        real = ref[:, 0, kk].reshape(len(dxs) * part, width)
        imag = ref[:, 1, kk].reshape(len(dxs) * part, width)
        s_real = dot(real, u_real) - dot(imag, u_imag)
        s_imag = dot(real, u_imag) + dot(imag, u_real)
        for n, dx in enumerate(dxs):
            for o in range(0, part, sub):
                live = struct_ref[node, (col ^ dx) * slots + (first + o) // width] >= 0
                at = pl.ds(pl.multiple_of(first + o, sub), sub)
                for plane, value in ((0, s_real), (1, s_imag)):
                    piece = value[n * part + o : n * part + o + sub]
                    out[plane, kk, dx - at_dx, at, :] = jnp.where(live, piece, 0.0).astype(BF16)


def scale_all(struct_ref, u_ref, refs, offsets, dxs, out, at_dx):
    row = lax.axis_index("prow")
    if offsets is None:

        @pl.loop(0, lax.axis_size("prow"))
        def _(member):
            scale(struct_ref, u_ref, refs[0].at[member], dxs, member, out, at_dx)

    else:
        for ref, dz in zip(refs, offsets, strict=True):
            scale(struct_ref, u_ref, ref, dxs, row ^ dz, out, at_dx)


def add_products(acc, ainv_ref, scaled, kk, here, at_dx):
    a_real, a_imag = ainv_ref[0, kk, here, :], ainv_ref[1, kk, here, :]
    s_real, s_imag = scaled[0, kk, at_dx], scaled[1, kk, at_dx]
    real, imag = acc
    real += dot(a_real, s_real) - dot(a_imag, s_imag)
    imag += dot(a_real, s_imag) + dot(a_imag, s_real)
    return real, imag


def solve_early(structure, u_inv, groups, near, ainv, rows):
    n_cols = lax.axis_size("pcol")
    own_k, _, width = groups[0][0][0].shape[-3:]
    arrays = [a for refs, _, _ in groups for a in refs]
    length = rows.group_slots * width

    def kernel(struct_ref, u_ref, *refs):
        group_refs, refs = refs[: len(arrays)], refs[len(arrays) :]
        ainv_refs, (scaled, acc_ref) = refs[: len(near)], refs[len(near) :]
        for values, offsets, dxs in groups:
            scale_all(struct_ref, u_ref, group_refs[: len(values)], offsets, dxs, scaled, 0)
            group_refs = group_refs[len(values) :]
        for kk in range(own_k):
            for i in range(rows.count):
                here = slice(i * width, (i + 1) * width)
                acc = jnp.zeros((width, width), F32), jnp.zeros((width, width), F32)
                for ref, dx in zip(ainv_refs, near, strict=True):
                    acc = add_products(acc, ref, scaled, kk, here, dx)
                acc_ref[0, kk, here, :], acc_ref[1, kk, here, :] = acc

    outs = [
        jax.ShapeDtypeStruct((2, own_k, n_cols, length, width), BF16),
        jax.ShapeDtypeStruct((2, own_k, rows.count * width, width), F32),
    ]
    inputs = [u_inv, *arrays, *[ainv[dx] for dx in near]]
    return pl.pallas_call(
        kernel,
        name="solve_early",
        in_specs=[SMEM] + [VMEM] * len(inputs),
        out_specs=[VMEM] * 2,
        out_shape=outs,
        compiler_params=limits(*outs, *inputs),
    )(structure, *inputs)


def solve_late(structure, u_inv, last, scaled, acc, far, ainv, rows):
    n_rows = lax.axis_size("prow")
    _, own_k, _, width = acc.shape
    values, offsets, dxs = last
    few = offsets is not None
    band = width // n_rows

    def kernel(struct_ref, u_ref, scaled_ref, acc_ref, *refs):
        last_refs, refs = refs[: len(values)], refs[len(values) :]
        ainv_refs, refs = refs[: len(far)], refs[len(far) :]
        sel_ref, *q_refs, scaled, quad = refs
        col, row = lax.axis_index("pcol"), lax.axis_index("prow")
        scaled[...] = scaled_ref[:, :, far[0] :]
        scale_all(struct_ref, u_ref, last_refs, offsets, dxs, scaled, far[0])
        for kk in range(own_k):
            node = col * own_k + kk
            q_real = jnp.zeros((width, width), F32)
            q_imag = jnp.zeros((width, width), F32)
            for i in range(rows.count):
                _, live, group, slot = rows.entry(struct_ref, node, row, i)
                here = slice(i * width, (i + 1) * width)
                acc = acc_ref[0, kk, here, :], acc_ref[1, kk, here, :]
                for ref, dx in zip(ainv_refs, far, strict=True):
                    acc = add_products(acc, ref, scaled, kk, here, dx - far[0])
                sel_real = jnp.where(live, -acc[0], 0.0)
                sel_imag = jnp.where(live, -acc[1], 0.0)
                sel_ref[0, kk, here, :], sel_ref[1, kk, here, :] = sel_real, sel_imag
                at = pl.ds(pl.multiple_of(slot * width, width), width)
                dx = group ^ col
                is_far = dx >= far[0]
                fdx = jnp.where(is_far, dx - far[0], 0)
                left_real = jnp.where(is_far, scaled[0, kk, fdx, at, :], scaled_ref[0, kk, dx, at, :])
                left_imag = jnp.where(is_far, scaled[1, kk, fdx, at, :], scaled_ref[1, kk, dx, at, :])
                hi_real, hi_imag = sel_real.astype(BF16), sel_imag.astype(BF16)
                lo_real = (sel_real - hi_real.astype(F32)).astype(BF16)
                lo_imag = (sel_imag - hi_imag.astype(F32)).astype(BF16)
                right = jnp.concatenate([hi_real, hi_imag, lo_real, lo_imag], axis=1)
                by_real, by_imag = tdot(left_real, right), tdot(left_imag, right)
                by_real = by_real[:, : 2 * width] + by_real[:, 2 * width :]
                by_imag = by_imag[:, : 2 * width] + by_imag[:, 2 * width :]
                q_real += by_real[:, :width] - by_imag[:, width:]
                q_imag += by_real[:, width:] + by_imag[:, :width]
            quad[0], quad[1] = q_real, q_imag
            for plane in range(2):
                if few:
                    for dz in range(n_rows):
                        at = pl.ds(pl.multiple_of((row ^ dz) * band, band), band)
                        q_refs[dz][plane, kk] = quad[plane, at, :].astype(q_refs[dz].dtype)
                else:
                    q_refs[0][plane, kk] = quad[plane].astype(BF16)

    chunk = (2, own_k, band, width)
    if few:
        terms = [jax.ShapeDtypeStruct(chunk, F32)] + [jax.ShapeDtypeStruct(chunk, BF16)] * (n_rows - 1)
    else:
        terms = [jax.ShapeDtypeStruct((2, own_k, width, width), BF16)]
    length = scaled.shape[3]
    late = jax.ShapeDtypeStruct((2, own_k, len(far), length, width), BF16)
    quad = jax.ShapeDtypeStruct((2, width, width), F32)
    inputs = [u_inv, scaled, acc, *values, *[ainv[dx] for dx in far]]
    out = pl.pallas_call(
        kernel,
        name="solve_late",
        in_specs=[SMEM] + [VMEM] * len(inputs),
        out_specs=[VMEM] * (1 + len(terms)),
        out_shape=[acc] + terms,
        scratch_shapes=[pltpu.VMEM(late.shape, late.dtype), pltpu.VMEM(quad.shape, quad.dtype)],
        compiler_params=limits(*terms, late, quad, acc, *inputs),
    )(structure, *inputs)
    return out[0], out[1:]


def place(structure, sel, rows):
    _, own_k, _, width = sel.shape

    def kernel(struct_ref, sel_ref, out_ref):
        col, row = lax.axis_index("pcol"), lax.axis_index("prow")
        if rows.by_slot:
            out_ref[...] = jnp.zeros_like(out_ref)
        for kk in range(own_k):
            for i in range(rows.count):
                block, live, _, _ = rows.entry(struct_ref, col * own_k + kk, row, i)

                def put(block=block, kk=kk, i=i):
                    at = pl.ds(pl.multiple_of(block * width, width), width)
                    out_ref[:, at, kk * width : (kk + 1) * width] = sel_ref[:, kk, i * width : (i + 1) * width, :]

                if rows.by_slot:
                    pl.when(live)(put)
                else:
                    put()

    out = jax.ShapeDtypeStruct((2, rows.row_blocks * width, own_k * width), F32)
    return pl.pallas_call(
        kernel,
        name="place",
        in_specs=[SMEM, VMEM],
        out_specs=VMEM,
        out_shape=out,
        compiler_params=limits(out, sel),
    )(structure, sel)


def finish_band(k_inv, terms):
    def kernel(k_ref, *refs):
        *term_refs, out_ref = refs
        row = lax.axis_index("prow")
        band = out_ref.shape[2]
        total = term_refs[0][...].astype(F32)
        for ref in term_refs[1:]:
            total += ref[...].astype(F32)
        at = pl.ds(pl.multiple_of(row * band, band), band)
        out_ref[...] = (k_ref[:, :, at, :] - total).astype(BF16)

    return pl.pallas_call(
        kernel,
        name="finish_band",
        in_specs=[VMEM] * (1 + len(terms)),
        out_specs=VMEM,
        out_shape=jax.ShapeDtypeStruct(terms[0].shape, BF16),
        compiler_params=limits(k_inv, *terms),
    )(k_inv, *terms)


def join_bands(bands, shape):
    def kernel(*refs):
        *band_refs, out_ref = refs
        row = lax.axis_index("prow")
        band = band_refs[0].shape[2]
        for d, ref in enumerate(band_refs):
            at = pl.ds(pl.multiple_of((row ^ d) * band, band), band)
            out_ref[:, :, at, :] = ref[...].astype(F32)

    return pl.pallas_call(
        kernel,
        name="join_bands",
        in_specs=[VMEM] * len(bands),
        out_specs=VMEM,
        out_shape=jax.ShapeDtypeStruct(shape, F32),
        compiler_params=limits(jax.ShapeDtypeStruct(shape, F32), *bands),
    )(*bands)


def gather_rows(x):
    n = lax.axis_size("prow")
    if n > FEW:
        return [lax.all_gather(x, "prow")], None
    held = {0: x}
    d = n // 2
    while d:
        held.update({at ^ d: swap(value, "prow", d) for at, value in list(held.items())})
        d //= 2
    return [held[d] for d in range(n)], list(range(n))


def local(ainv_anc, panel, u_inv, k_inv, structure):
    width = u_inv.shape[-1]
    own_k = k_inv.shape[1]
    n_rows, n_cols = lax.axis_size("prow"), lax.axis_size("pcol")
    rows = Rows(ainv_anc.shape[1] // width, ainv_anc.shape[2] // width, structure.shape[1] // n_cols)
    parts = pick_panel(panel, own_k)
    parts = [parts[0]] + [swap(parts[d], "pcol", d) for d in range(1, n_cols)]
    near, far = list(range(n_cols // 2)), list(range(n_cols // 2, n_cols))
    groups = []
    for dxs in [[d] for d in near] + [far]:
        values = jnp.stack([parts[d] for d in dxs])
        groups.append((*gather_rows(values), dxs))
    blocks = pick_ainv(ainv_anc, structure, own_k, width, rows)
    ainv = [blocks[0]] + [swap(blocks[d], "pcol", d) for d in range(1, n_cols)]
    values, offsets, dxs = groups.pop()
    if offsets is None:
        last = (values, None, dxs)
    else:
        groups.append((values[:-1], offsets[:-1], dxs))
        last = (values[-1:], offsets[-1:], dxs)
    scaled, acc = solve_early(structure, u_inv, groups, near, ainv, rows)
    sel, terms = solve_late(structure, u_inv, last, scaled, acc, far, ainv, rows)
    sel_inv = place(structure, sel, rows)
    if n_rows > FEW:
        total = lax.psum_scatter(terms[0], "prow", scatter_dimension=2, tiled=True)
        mine = finish_band(k_inv, [total])
        return sel_inv, lax.all_gather(mine, "prow", axis=2, tiled=True).astype(F32)
    terms = [terms[0]] + [swap(terms[d], "prow", d) for d in range(1, n_rows)]
    mine = finish_band(k_inv, terms)
    bands = [mine] + [swap(mine, "prow", d) for d in range(1, n_rows)]
    return sel_inv, join_bands(bands, k_inv.shape)


def solution(mesh):
    placed = (
        P(None, ("pole", "prow"), "pcol"),
        P(None, "pole", ("pcol", "prow"), None),
        P(None, "pole", None, None),
        P(None, ("pole", "pcol"), None, None),
        P(),
    )
    return jax.shard_map(
        local,
        mesh=mesh,
        in_specs=placed,
        out_specs=(P(None, ("pole", "prow"), "pcol"), P(None, ("pole", "pcol"), None, None)),
        check_vma=False,
    )
```

```python
import jax
import jax.numpy as jnp
from jax import lax
from jax.experimental import pallas as pl
from jax.experimental.pallas import tpu as pltpu
from jax.sharding import PartitionSpec as P

BF16 = jnp.bfloat16
F32 = jnp.float32
NEAR = 1
FEW = 8
HBM = pl.BlockSpec(memory_space=pltpu.HBM)
VMEM = pl.BlockSpec(memory_space=pltpu.VMEM)
SMEM = pl.BlockSpec(memory_space=pltpu.SMEM)


def swap(x, axis, d):
    n = lax.axis_size(axis)
    return lax.ppermute(x, axis, [(i, i ^ d) for i in range(n)])


def nbytes(*arrays):
    return sum(a.size * a.dtype.itemsize for a in arrays)


def limits(*arrays):
    return pltpu.CompilerParams(vmem_limit_bytes=nbytes(*arrays) + (4 << 20))


class Rows:
    def __init__(self, row_blocks, group_blocks, group_slots):
        self.row_blocks, self.group_blocks, self.group_slots = row_blocks, group_blocks, group_slots
        nested = row_blocks % group_blocks == 0 or group_blocks % row_blocks == 0
        slots = max(row_blocks // group_blocks, 1) * group_slots
        self.by_slot = nested and slots < row_blocks
        self.count = slots if self.by_slot else row_blocks

    def slot_of(self, row, index):
        slot = (row * self.row_blocks // self.group_blocks) * self.group_slots + index
        return slot // self.group_slots, slot % self.group_slots

    def entry(self, struct_ref, node, row, index):
        base = row * self.row_blocks
        if self.by_slot:
            slot = (base // self.group_blocks) * self.group_slots + index
            block = struct_ref[node, slot] - base
            live = jnp.logical_and(block >= 0, block < self.row_blocks)
            return jnp.where(live, block, 0), live, slot // self.group_slots, slot % self.group_slots
        target = base + index
        group = target // self.group_blocks
        found, live = jnp.int32(0), jnp.int32(0)
        for s in range(self.group_slots):
            hit = struct_ref[node, group * self.group_slots + s] == target
            found = jnp.where(hit, s, found)
            live = jnp.where(hit, 1, live)
        return jnp.int32(index), live > 0, group, found


def run_copies(copies):
    for copy in copies:
        copy.start()
    for copy in copies:
        copy.wait()


def pick_panel(panel, own_k):
    n_cols = lax.axis_size("pcol")

    def kernel(panel_ref, *refs):
        outs, sems = refs[:-1], refs[-1]
        col = lax.axis_index("pcol")
        sources = [panel_ref.at[:, pl.ds((col ^ d) * own_k, own_k)] for d in range(n_cols)]
        run_copies([pltpu.make_async_copy(sources[d], outs[d], sems.at[d]) for d in range(n_cols)])

    planes, _, part, width = panel.shape
    outs = [jax.ShapeDtypeStruct((planes, own_k, part, width), panel.dtype)] * n_cols
    return pl.pallas_call(
        kernel,
        name="pick_panel",
        in_specs=[HBM],
        out_specs=[VMEM] * n_cols,
        out_shape=outs,
        scratch_shapes=[pltpu.SemaphoreType.DMA((n_cols,))],
        compiler_params=limits(*outs),
    )(pltpu.with_memory_space_constraint(panel, pltpu.HBM))


def pick_ainv(ainv, structure, own_k, width, rows, ds):
    slots = rows.group_slots

    def kernel(struct_ref, ainv_ref, *refs):
        outs, sems = refs[: len(ds)], refs[len(ds)]
        col, row = lax.axis_index("pcol"), lax.axis_index("prow")
        copies = []
        for n, d in enumerate(ds):
            for kk in range(own_k):
                node = (col ^ d) * own_k + kk
                for i in range(rows.count):
                    block, _, _, _ = rows.entry(struct_ref, node, row, i)
                    for s in range(slots):
                        j = struct_ref[node, col * slots + s] - col * rows.group_blocks
                        j = jnp.maximum(j, 0)
                        copies.append(
                            pltpu.make_async_copy(
                                ainv_ref.at[:, pl.ds(block * width, width), pl.ds(j * width, width)],
                                outs[n].at[:, kk, pl.ds(i * width, width), pl.ds(s * width, width)],
                                sems.at[n, kk, i, s],
                            )
                        )
        run_copies(copies)

    outs = [jax.ShapeDtypeStruct((2, own_k, rows.count * width, slots * width), ainv.dtype)] * len(ds)
    return pl.pallas_call(
        kernel,
        name="pick_ainv",
        in_specs=[SMEM, HBM],
        out_specs=[VMEM] * len(ds),
        out_shape=outs,
        scratch_shapes=[pltpu.SemaphoreType.DMA((len(ds), own_k, rows.count, slots))],
        compiler_params=limits(*outs),
    )(structure, pltpu.with_memory_space_constraint(ainv, pltpu.HBM))


def dot(left, right):
    return jnp.dot(left, right, preferred_element_type=F32)


def tdot(left, right):
    return lax.dot_general(left, right, (((0,), (0,)), ((), ())), preferred_element_type=F32)


def scale(is_live, u_ref, ref, dxs, member, out):
    col = lax.axis_index("pcol")
    _, _, own_k, part, width = ref.shape
    sub = min(part, width)
    first = member * part
    for kk in range(own_k):
        u_real, u_imag = u_ref[0, col * own_k + kk], u_ref[1, col * own_k + kk]
        real = ref[:, 0, kk].reshape(len(dxs) * part, width)
        imag = ref[:, 1, kk].reshape(len(dxs) * part, width)
        s_real = dot(real, u_real) - dot(imag, u_imag)
        s_imag = dot(real, u_imag) + dot(imag, u_real)
        for n, dx in enumerate(dxs):
            for o in range(0, part, sub):
                live = is_live(kk, dx, (first + o) // width)
                at = pl.ds(pl.multiple_of(first + o, sub), sub)
                for plane, value in ((0, s_real), (1, s_imag)):
                    piece = value[n * part + o : n * part + o + sub]
                    out(plane, kk, dx)[at, :] = jnp.where(live, piece, 0.0).astype(BF16)


def scale_all(is_live, u_ref, refs, offsets, dxs, out):
    row = lax.axis_index("prow")
    if offsets is None:

        @pl.loop(0, lax.axis_size("prow"))
        def _(member):
            scale(is_live, u_ref, refs[0].at[member], dxs, member, out)

    else:
        for ref, dz in zip(refs, offsets, strict=True):
            scale(is_live, u_ref, ref, dxs, row ^ dz, out)


def take(refs, groups):
    dealt = []
    for values, offsets, dxs in groups:
        dealt.append((refs[: len(values)], offsets, dxs))
        refs = refs[len(values) :]
    return dealt, refs


def add_products(acc, ainv_ref, s_real, s_imag, kk, here):
    a_real, a_imag = ainv_ref[0, kk, here, :], ainv_ref[1, kk, here, :]
    real, imag = acc
    real += dot(a_real, s_real) - dot(a_imag, s_imag)
    imag += dot(a_real, s_imag) + dot(a_imag, s_real)
    return real, imag


def solve_early(structure, u_inv, groups, near, ainv, rows):
    n_cols = lax.axis_size("pcol")
    own_k, _, width = groups[0][0][0].shape[-3:]
    slots = rows.group_slots

    def kernel(struct_ref, u_ref, *refs):
        col, row = lax.axis_index("pcol"), lax.axis_index("prow")
        dealt, refs = take(refs, groups)
        ainv_refs, (scaled, acc_ref, slot_mask, row_mask) = refs[: len(near)], refs[len(near) :]
        for kk in range(own_k):
            node = col * own_k + kk
            for dx in range(n_cols):
                for s in range(slots):
                    live = struct_ref[node, (col ^ dx) * slots + s] >= 0
                    slot_mask[kk, dx, s] = jnp.full((8, width), jnp.where(live, 1.0, 0.0), F32)
            for i in range(rows.count):
                _, live, _, _ = rows.entry(struct_ref, node, row, i)
                row_mask[kk, i] = jnp.full((8, width), jnp.where(live, 1.0, 0.0), F32)

        def is_live(kk, dx, slot):
            return struct_ref[col * own_k + kk, (col ^ dx) * slots + slot] >= 0

        for values, offsets, dxs in dealt:
            scale_all(is_live, u_ref, values, offsets, dxs, lambda plane, kk, dx: scaled.at[plane, kk, dx])
        for kk in range(own_k):
            for i in range(rows.count):
                here = slice(i * width, (i + 1) * width)
                acc = jnp.zeros((width, width), F32), jnp.zeros((width, width), F32)
                for ref, dx in zip(ainv_refs, near, strict=True):
                    acc = add_products(acc, ref, scaled[0, kk, dx], scaled[1, kk, dx], kk, here)
                acc_ref[0, kk, here, :], acc_ref[1, kk, here, :] = acc

    outs = [
        jax.ShapeDtypeStruct((2, own_k, n_cols, slots * width, width), BF16),
        jax.ShapeDtypeStruct((2, own_k, rows.count * width, width), F32),
        jax.ShapeDtypeStruct((own_k, n_cols, slots, 8, width), F32),
        jax.ShapeDtypeStruct((own_k, rows.count, 8, width), F32),
    ]
    inputs = [u_inv, *[a for values, _, _ in groups for a in values], *[ainv[dx] for dx in near]]
    return pl.pallas_call(
        kernel,
        name="solve_early",
        in_specs=[SMEM] + [VMEM] * len(inputs),
        out_specs=[VMEM] * len(outs),
        out_shape=outs,
        compiler_params=limits(*outs, *inputs),
    )(structure, *inputs)


def solve_late(structure, u_inv, groups, early, far, ainv, rows):
    n_rows = lax.axis_size("prow")
    scaled, acc, _, _ = early
    _, own_k, _, width = acc.shape
    few = groups[-1][1] is not None
    band = width // n_rows
    struct = [] if rows.by_slot else [structure]

    def kernel(*refs):
        struct_refs, refs = refs[: len(struct)], refs[len(struct) :]
        (u_ref, scaled_ref, acc_ref, slot_mask, row_mask), refs = refs[:5], refs[5:]
        dealt, refs = take(refs, groups)
        ainv_refs, refs = refs[: len(far)], refs[len(far) :]
        sel_ref, *q_refs, scaled, quad = refs
        col, row = lax.axis_index("pcol"), lax.axis_index("prow")

        def is_live(kk, dx, slot):
            return slot_mask[kk, dx, slot, 0:1, :] > 0.0

        scaled[...] = scaled_ref[...]
        for values, offsets, dxs in dealt:
            scale_all(is_live, u_ref, values, offsets, dxs, lambda plane, kk, dx: scaled.at[plane, kk, dx])
        for kk in range(own_k):
            q_real = jnp.zeros((width, width), F32)
            q_imag = jnp.zeros((width, width), F32)
            for i in range(rows.count):
                if rows.by_slot:
                    group, slot = rows.slot_of(row, i)
                else:
                    _, _, group, slot = rows.entry(struct_refs[0], col * own_k + kk, row, i)
                live = row_mask[kk, i, 0:1, :] > 0.0
                here = slice(i * width, (i + 1) * width)
                acc = acc_ref[0, kk, here, :], acc_ref[1, kk, here, :]
                for ref, dx in zip(ainv_refs, far, strict=True):
                    acc = add_products(acc, ref, scaled[0, kk, dx], scaled[1, kk, dx], kk, here)
                sel_real = jnp.where(live, -acc[0], 0.0)
                sel_imag = jnp.where(live, -acc[1], 0.0)
                sel_ref[0, kk, here, :], sel_ref[1, kk, here, :] = sel_real, sel_imag
                at = pl.ds(pl.multiple_of(slot * width, width), width)
                left_real, left_imag = scaled[0, kk, group ^ col, at, :], scaled[1, kk, group ^ col, at, :]
                hi_real, hi_imag = sel_real.astype(BF16), sel_imag.astype(BF16)
                lo_real = (sel_real - hi_real.astype(F32)).astype(BF16)
                lo_imag = (sel_imag - hi_imag.astype(F32)).astype(BF16)
                right = jnp.concatenate([hi_real, hi_imag, lo_real, lo_imag], axis=1)
                by_real, by_imag = tdot(left_real, right), tdot(left_imag, right)
                by_real = by_real[:, : 2 * width] + by_real[:, 2 * width :]
                by_imag = by_imag[:, : 2 * width] + by_imag[:, 2 * width :]
                q_real += by_real[:, :width] - by_imag[:, width:]
                q_imag += by_real[:, width:] + by_imag[:, :width]
            quad[0], quad[1] = q_real, q_imag
            for plane in range(2):
                if few:
                    for dz in range(n_rows):
                        at = pl.ds(pl.multiple_of((row ^ dz) * band, band), band)
                        q_refs[dz][plane, kk] = quad[plane, at, :].astype(q_refs[dz].dtype)
                else:
                    q_refs[0][plane, kk] = quad[plane].astype(BF16)

    chunk = (2, own_k, band, width)
    if few:
        terms = [jax.ShapeDtypeStruct(chunk, F32)] + [jax.ShapeDtypeStruct(chunk, BF16)] * (n_rows - 1)
    else:
        terms = [jax.ShapeDtypeStruct((2, own_k, width, width), BF16)]
    quad = jax.ShapeDtypeStruct((2, width, width), F32)
    inputs = [u_inv, *early, *[a for values, _, _ in groups for a in values], *[ainv[dx] for dx in far]]
    out = pl.pallas_call(
        kernel,
        name="solve_late",
        in_specs=[SMEM] * len(struct) + [VMEM] * len(inputs),
        out_specs=[VMEM] * (1 + len(terms)),
        out_shape=[acc] + terms,
        scratch_shapes=[pltpu.VMEM(scaled.shape, scaled.dtype), pltpu.VMEM(quad.shape, quad.dtype)],
        compiler_params=limits(*terms, scaled, quad, acc, *inputs),
    )(*struct, *inputs)
    return out[0], out[1:]


def place(structure, sel, rows):
    _, own_k, _, width = sel.shape

    def kernel(struct_ref, sel_ref, out_ref):
        col, row = lax.axis_index("pcol"), lax.axis_index("prow")
        if rows.by_slot:
            out_ref[...] = jnp.zeros_like(out_ref)
        for kk in range(own_k):
            for i in range(rows.count):
                block, live, _, _ = rows.entry(struct_ref, col * own_k + kk, row, i)

                def put(block=block, kk=kk, i=i):
                    at = pl.ds(pl.multiple_of(block * width, width), width)
                    out_ref[:, at, kk * width : (kk + 1) * width] = sel_ref[:, kk, i * width : (i + 1) * width, :]

                if rows.by_slot:
                    pl.when(live)(put)
                else:
                    put()

    out = jax.ShapeDtypeStruct((2, rows.row_blocks * width, own_k * width), F32)
    return pl.pallas_call(
        kernel,
        name="place",
        in_specs=[SMEM, VMEM],
        out_specs=VMEM,
        out_shape=out,
        compiler_params=limits(out, sel),
    )(structure, sel)


def finish_band(k_inv, terms):
    def kernel(k_ref, *refs):
        *term_refs, out_ref = refs
        row = lax.axis_index("prow")
        band = out_ref.shape[2]
        total = term_refs[0][...].astype(F32)
        for ref in term_refs[1:]:
            total += ref[...].astype(F32)
        at = pl.ds(pl.multiple_of(row * band, band), band)
        out_ref[...] = (k_ref[:, :, at, :] - total).astype(BF16)

    return pl.pallas_call(
        kernel,
        name="finish_band",
        in_specs=[VMEM] * (1 + len(terms)),
        out_specs=VMEM,
        out_shape=jax.ShapeDtypeStruct(terms[0].shape, BF16),
        compiler_params=limits(k_inv, *terms),
    )(k_inv, *terms)


def join_bands(bands, shape):
    def kernel(*refs):
        *band_refs, out_ref = refs
        row = lax.axis_index("prow")
        band = band_refs[0].shape[2]
        for d, ref in enumerate(band_refs):
            at = pl.ds(pl.multiple_of((row ^ d) * band, band), band)
            out_ref[:, :, at, :] = ref[...].astype(F32)

    return pl.pallas_call(
        kernel,
        name="join_bands",
        in_specs=[VMEM] * len(bands),
        out_specs=VMEM,
        out_shape=jax.ShapeDtypeStruct(shape, F32),
        compiler_params=limits(jax.ShapeDtypeStruct(shape, F32), *bands),
    )(*bands)


def gather_rows(x, direct):
    n = lax.axis_size("prow")
    if n > FEW:
        return [lax.all_gather(x, "prow")], None
    if direct:
        return [x] + [swap(x, "prow", d) for d in range(1, n)], list(range(n))
    held = {0: x}
    d = n // 2
    while d:
        held.update({at ^ d: swap(value, "prow", d) for at, value in list(held.items())})
        d //= 2
    return [held[d] for d in range(n)], list(range(n))


def groups_of(n_cols):
    half = n_cols // 2
    return [[d] for d in range(half)] + [list(range(half, n_cols))]


def local(ainv_anc, panel, u_inv, k_inv, structure):
    width = u_inv.shape[-1]
    own_k = k_inv.shape[1]
    n_rows, n_cols = lax.axis_size("prow"), lax.axis_size("pcol")
    rows = Rows(ainv_anc.shape[1] // width, ainv_anc.shape[2] // width, structure.shape[1] // n_cols)
    parts = pick_panel(panel, own_k)
    parts = [parts[0]] + [swap(parts[d], "pcol", d) for d in range(1, n_cols)]
    near, far = list(range(NEAR)), list(range(NEAR, n_cols))
    near_a, far_a = list(range(n_cols // 2)), list(range(n_cols // 2, n_cols))
    groups = []
    for dxs in groups_of(n_cols):
        values = jnp.stack([parts[d] for d in dxs])
        groups.append((*gather_rows(values, False), dxs))
    blocks = dict(zip(far_a, pick_ainv(ainv_anc, structure, own_k, width, rows, far_a), strict=True))
    blocks.update(zip(near_a, pick_ainv(ainv_anc, structure, own_k, width, rows, near_a), strict=True))
    ainv = [blocks[0]] + [swap(blocks[d], "pcol", d) for d in range(1, n_cols)]
    early, late = [], []
    for values, offsets, dxs in groups:
        whole = set(dxs) <= set(near)
        if whole or offsets is None:
            (early if whole else late).append((values, offsets, dxs))
        else:
            early.append((values[:-1], offsets[:-1], dxs))
            late.append((values[-1:], offsets[-1:], dxs))
    found = solve_early(structure, u_inv, early, near, ainv, rows)
    sel, terms = solve_late(structure, u_inv, late, found, far, ainv, rows)
    sel_inv = place(structure, sel, rows)
    if n_rows > FEW:
        total = lax.psum_scatter(terms[0], "prow", scatter_dimension=2, tiled=True)
        mine = finish_band(k_inv, [total])
        return sel_inv, lax.all_gather(mine, "prow", axis=2, tiled=True).astype(F32)
    terms = [terms[0]] + [swap(terms[d], "prow", d) for d in range(1, n_rows)]
    mine = finish_band(k_inv, terms)
    bands, _ = gather_rows(mine, True)
    return sel_inv, join_bands(bands, k_inv.shape)


def solution(mesh):
    placed = (
        P(None, ("pole", "prow"), "pcol"),
        P(None, "pole", ("pcol", "prow"), None),
        P(None, "pole", None, None),
        P(None, ("pole", "pcol"), None, None),
        P(),
    )
    return jax.shard_map(
        local,
        mesh=mesh,
        in_specs=placed,
        out_specs=(P(None, ("pole", "prow"), "pcol"), P(None, ("pole", "pcol"), None, None)),
        check_vma=False,
    )
```

```python
import jax
import jax.numpy as jnp
from jax import lax
from jax.experimental import pallas as pl
from jax.experimental.pallas import tpu as pltpu
from jax.sharding import PartitionSpec as P

BF16 = jnp.bfloat16
F32 = jnp.float32
FEW = 8
HBM = pl.BlockSpec(memory_space=pltpu.HBM)
VMEM = pl.BlockSpec(memory_space=pltpu.VMEM)
SMEM = pl.BlockSpec(memory_space=pltpu.SMEM)


def swap(x, axis, d):
    n = lax.axis_size(axis)
    return lax.ppermute(x, axis, [(i, i ^ d) for i in range(n)])


def turn(x, k):
    n = lax.axis_size("prow")
    return lax.ppermute(x, "prow", [(i, (i + k) % n) for i in range(n)])


def member(k):
    n = lax.axis_size("prow")
    return lax.rem(lax.axis_index("prow") + (k + n) % n, n)


def nbytes(*arrays):
    return sum(a.size * a.dtype.itemsize for a in arrays)


def limits(*arrays):
    return pltpu.CompilerParams(vmem_limit_bytes=nbytes(*arrays) + (4 << 20))


class Rows:
    def __init__(self, row_blocks, group_blocks, group_slots):
        self.row_blocks, self.group_blocks, self.group_slots = row_blocks, group_blocks, group_slots
        nested = row_blocks % group_blocks == 0 or group_blocks % row_blocks == 0
        slots = max(row_blocks // group_blocks, 1) * group_slots
        self.by_slot = nested and slots < row_blocks
        self.count = slots if self.by_slot else row_blocks

    def slot_of(self, row, index):
        slot = (row * self.row_blocks // self.group_blocks) * self.group_slots + index
        return slot // self.group_slots, slot % self.group_slots

    def entry(self, struct_ref, node, row, index):
        base = row * self.row_blocks
        if self.by_slot:
            slot = (base // self.group_blocks) * self.group_slots + index
            block = struct_ref[node, slot] - base
            live = jnp.logical_and(block >= 0, block < self.row_blocks)
            return jnp.where(live, block, 0), live, slot // self.group_slots, slot % self.group_slots
        target = base + index
        group = target // self.group_blocks
        found, live = jnp.int32(0), jnp.int32(0)
        for s in range(self.group_slots):
            hit = struct_ref[node, group * self.group_slots + s] == target
            found = jnp.where(hit, s, found)
            live = jnp.where(hit, 1, live)
        return jnp.int32(index), live > 0, group, found


def run_copies(copies):
    for copy in copies:
        copy.start()
    for copy in copies:
        copy.wait()


def pick_panel(panel, structure, own_k):
    n_cols = lax.axis_size("pcol")

    def kernel(panel_ref, struct_ref, *refs):
        outs, sems = refs[:-1], refs[-1]
        col = lax.axis_index("pcol")
        sources = [panel_ref.at[:, pl.ds((col ^ d) * own_k, own_k)] for d in range(n_cols)] + [struct_ref]
        run_copies([pltpu.make_async_copy(sources[i], outs[i], sems.at[i]) for i in range(len(outs))])

    planes, _, part, width = panel.shape
    outs = [jax.ShapeDtypeStruct((planes, own_k, part, width), panel.dtype)] * n_cols
    outs += [jax.ShapeDtypeStruct(structure.shape, structure.dtype)]
    out = pl.pallas_call(
        kernel,
        name="pick_panel",
        in_specs=[HBM] * 2,
        out_specs=[VMEM] * len(outs),
        out_shape=outs,
        scratch_shapes=[pltpu.SemaphoreType.DMA((len(outs),))],
        compiler_params=limits(*outs),
    )(*[pltpu.with_memory_space_constraint(x, pltpu.HBM) for x in (panel, structure)])
    return out[:-1], out[-1]


def pick_ainv(ainv, structure, own_k, width, rows, ds):
    slots = rows.group_slots

    def kernel(struct_ref, ainv_ref, *refs):
        outs, sems = refs[: len(ds)], refs[len(ds)]
        col, row = lax.axis_index("pcol"), lax.axis_index("prow")
        copies = []
        for n, d in enumerate(ds):
            for kk in range(own_k):
                node = (col ^ d) * own_k + kk
                for i in range(rows.count):
                    block, _, _, _ = rows.entry(struct_ref, node, row, i)
                    for s in range(slots):
                        j = struct_ref[node, col * slots + s] - col * rows.group_blocks
                        j = jnp.maximum(j, 0)
                        for plane in range(2):
                            copies.append(
                                pltpu.make_async_copy(
                                    ainv_ref.at[plane, pl.ds(block * width, width), pl.ds(j * width, width)],
                                    outs[n].at[plane, kk, pl.ds(i * width, width), pl.ds(s * width, width)],
                                    sems.at[n, kk, i, s, plane],
                                )
                            )
        run_copies(copies)

    outs = [jax.ShapeDtypeStruct((2, own_k, rows.count * width, slots * width), ainv.dtype)] * len(ds)
    return pl.pallas_call(
        kernel,
        name="pick_ainv",
        in_specs=[SMEM, HBM],
        out_specs=[VMEM] * len(ds),
        out_shape=outs,
        scratch_shapes=[pltpu.SemaphoreType.DMA((len(ds), own_k, rows.count, slots, 2))],
        compiler_params=limits(*outs),
    )(structure, pltpu.with_memory_space_constraint(ainv, pltpu.HBM))


def dot(left, right):
    return jnp.dot(left, right, preferred_element_type=F32)


def tdot(left, right):
    return lax.dot_general(left, right, (((0,), (0,)), ((), ())), preferred_element_type=F32)


def scale(is_live, u_ref, ref, dxs, member, out):
    col = lax.axis_index("pcol")
    _, _, own_k, part, width = ref.shape
    sub = min(part, width)
    first = member * part
    for kk in range(own_k):
        u_real, u_imag = u_ref[0, col * own_k + kk], u_ref[1, col * own_k + kk]
        real = ref[:, 0, kk].reshape(len(dxs) * part, width)
        imag = ref[:, 1, kk].reshape(len(dxs) * part, width)
        s_real = dot(real, u_real) - dot(imag, u_imag)
        s_imag = dot(real, u_imag) + dot(imag, u_real)
        for n, dx in enumerate(dxs):
            for o in range(0, part, sub):
                live = is_live(kk, dx, (first + o) // width)
                at = pl.ds(pl.multiple_of(first + o, sub), sub)
                for plane, value in ((0, s_real), (1, s_imag)):
                    piece = value[n * part + o : n * part + o + sub]
                    out(plane, kk, dx)[at, :] = jnp.where(live, piece, 0.0).astype(BF16)


def scale_all(is_live, u_ref, refs, offsets, dxs, out):
    row = lax.axis_index("prow")
    if offsets is None:

        @pl.loop(0, lax.axis_size("prow"))
        def _(member):
            scale(is_live, u_ref, refs[0].at[member], dxs, member, out)

    else:
        for ref, dz in zip(refs, offsets, strict=True):
            scale(is_live, u_ref, ref, dxs, row ^ dz, out)


def take(refs, groups):
    dealt = []
    for values, offsets, dxs in groups:
        dealt.append((refs[: len(values)], offsets, dxs))
        refs = refs[len(values) :]
    return dealt, refs


def add_products(acc, ainv_ref, s_real, s_imag, kk, here):
    a_real, a_imag = ainv_ref[0, kk, here, :], ainv_ref[1, kk, here, :]
    real, imag = acc
    real += dot(a_real, s_real) - dot(a_imag, s_imag)
    imag += dot(a_real, s_imag) + dot(a_imag, s_real)
    return real, imag


def solve_early(structure, u_inv, groups, near, ainv, rows):
    n_cols = lax.axis_size("pcol")
    own_k, _, width = groups[0][0][0].shape[-3:]
    slots = rows.group_slots

    def kernel(struct_ref, u_ref, *refs):
        col, row = lax.axis_index("pcol"), lax.axis_index("prow")
        dealt, refs = take(refs, groups)
        ainv_refs, (scaled, acc_ref, slot_mask, row_mask) = refs[: len(near)], refs[len(near) :]
        for kk in range(own_k):
            node = col * own_k + kk
            for dx in range(n_cols):
                for s in range(slots):
                    live = struct_ref[node, (col ^ dx) * slots + s] >= 0
                    slot_mask[kk, dx, s] = jnp.full((8, width), jnp.where(live, 1.0, 0.0), F32)
            for i in range(rows.count):
                _, live, _, _ = rows.entry(struct_ref, node, row, i)
                row_mask[kk, i] = jnp.full((8, width), jnp.where(live, 1.0, 0.0), F32)

        def is_live(kk, dx, slot):
            return struct_ref[col * own_k + kk, (col ^ dx) * slots + slot] >= 0

        for values, offsets, dxs in dealt:
            scale_all(is_live, u_ref, values, offsets, dxs, lambda plane, kk, dx: scaled.at[plane, kk, dx])
        for kk in range(own_k):
            for i in range(rows.count):
                here = slice(i * width, (i + 1) * width)
                acc = jnp.zeros((width, width), F32), jnp.zeros((width, width), F32)
                for ref, dx in zip(ainv_refs, near, strict=True):
                    acc = add_products(acc, ref, scaled[0, kk, dx], scaled[1, kk, dx], kk, here)
                acc_ref[0, kk, here, :], acc_ref[1, kk, here, :] = acc

    outs = [
        jax.ShapeDtypeStruct((2, own_k, n_cols, slots * width, width), BF16),
        jax.ShapeDtypeStruct((2, own_k, rows.count * width, width), F32),
        jax.ShapeDtypeStruct((own_k, n_cols, slots, 8, width), F32),
        jax.ShapeDtypeStruct((own_k, rows.count, 8, width), F32),
    ]
    inputs = [u_inv, *[a for values, _, _ in groups for a in values], *[ainv[dx] for dx in near]]
    return pl.pallas_call(
        kernel,
        name="solve_early",
        in_specs=[SMEM] + [VMEM] * len(inputs),
        out_specs=[VMEM] * len(outs),
        out_shape=outs,
        compiler_params=limits(*outs, *inputs),
    )(structure, *inputs)


def solve_late(structure, u_inv, groups, early, far, ainv, rows):
    n_rows = lax.axis_size("prow")
    scaled, acc, _, _ = early
    _, own_k, _, width = acc.shape
    few = groups[-1][1] is not None
    band = width // n_rows
    struct = [] if rows.by_slot else [structure]

    def kernel(*refs):
        struct_refs, refs = refs[: len(struct)], refs[len(struct) :]
        (u_ref, scaled_ref, acc_ref, slot_mask, row_mask), refs = refs[:5], refs[5:]
        dealt, refs = take(refs, groups)
        ainv_refs, refs = refs[: len(far)], refs[len(far) :]
        sel_ref, *q_refs, scaled, quad = refs
        col, row = lax.axis_index("pcol"), lax.axis_index("prow")

        def is_live(kk, dx, slot):
            return slot_mask[kk, dx, slot, 0:1, :] > 0.0

        scaled[...] = scaled_ref[...]
        for values, offsets, dxs in dealt:
            scale_all(is_live, u_ref, values, offsets, dxs, lambda plane, kk, dx: scaled.at[plane, kk, dx])
        for kk in range(own_k):
            q_real = jnp.zeros((width, width), F32)
            q_imag = jnp.zeros((width, width), F32)
            for i in range(rows.count):
                if rows.by_slot:
                    group, slot = rows.slot_of(row, i)
                else:
                    _, _, group, slot = rows.entry(struct_refs[0], col * own_k + kk, row, i)
                live = row_mask[kk, i, 0:1, :] > 0.0
                here = slice(i * width, (i + 1) * width)
                acc = acc_ref[0, kk, here, :], acc_ref[1, kk, here, :]
                for ref, dx in zip(ainv_refs, far, strict=True):
                    acc = add_products(acc, ref, scaled[0, kk, dx], scaled[1, kk, dx], kk, here)
                sel_real = jnp.where(live, -acc[0], 0.0)
                sel_imag = jnp.where(live, -acc[1], 0.0)
                sel_ref[0, kk, here, :], sel_ref[1, kk, here, :] = sel_real, sel_imag
                at = pl.ds(pl.multiple_of(slot * width, width), width)
                left_real, left_imag = scaled[0, kk, group ^ col, at, :], scaled[1, kk, group ^ col, at, :]
                hi_real, hi_imag = sel_real.astype(BF16), sel_imag.astype(BF16)
                lo_real = (sel_real - hi_real.astype(F32)).astype(BF16)
                lo_imag = (sel_imag - hi_imag.astype(F32)).astype(BF16)
                right = jnp.concatenate([hi_real, hi_imag, lo_real, lo_imag], axis=1)
                by_real, by_imag = tdot(left_real, right), tdot(left_imag, right)
                by_real = by_real[:, : 2 * width] + by_real[:, 2 * width :]
                by_imag = by_imag[:, : 2 * width] + by_imag[:, 2 * width :]
                q_real += by_real[:, :width] - by_imag[:, width:]
                q_imag += by_real[:, width:] + by_imag[:, :width]
            quad[0], quad[1] = q_real, q_imag
            for plane in range(2):
                if few:
                    for k, q_ref in enumerate(q_refs):
                        at = pl.ds(pl.multiple_of(member(k) * band, band), band)
                        q_ref[plane, kk] = quad[plane, at, :].astype(q_ref.dtype)
                else:
                    q_refs[0][plane, kk] = quad[plane]

    chunk = (2, own_k, band, width)
    if few:
        terms = [jax.ShapeDtypeStruct(chunk, F32)] + [jax.ShapeDtypeStruct(chunk, BF16)] * (n_rows - 1)
    else:
        terms = [jax.ShapeDtypeStruct((2, own_k, width, width), F32)]
    quad = jax.ShapeDtypeStruct((2, width, width), F32)
    inputs = [u_inv, *early, *[a for values, _, _ in groups for a in values], *[ainv[dx] for dx in far]]
    out = pl.pallas_call(
        kernel,
        name="solve_late",
        in_specs=[SMEM] * len(struct) + [VMEM] * len(inputs),
        out_specs=[VMEM] * (1 + len(terms)),
        out_shape=[acc] + terms,
        scratch_shapes=[pltpu.VMEM(scaled.shape, scaled.dtype), pltpu.VMEM(quad.shape, quad.dtype)],
        compiler_params=limits(*terms, scaled, quad, acc, *inputs),
    )(*struct, *inputs)
    return out[0], out[1:]


def place(structure, sel, rows):
    _, own_k, _, width = sel.shape

    def kernel(struct_ref, sel_ref, out_ref):
        col, row = lax.axis_index("pcol"), lax.axis_index("prow")
        if rows.by_slot:
            out_ref[...] = jnp.zeros_like(out_ref)
        for kk in range(own_k):
            for i in range(rows.count):
                block, live, _, _ = rows.entry(struct_ref, col * own_k + kk, row, i)

                def put(block=block, kk=kk, i=i):
                    at = pl.ds(pl.multiple_of(block * width, width), width)
                    out_ref[:, at, kk * width : (kk + 1) * width] = sel_ref[:, kk, i * width : (i + 1) * width, :]

                if rows.by_slot:
                    pl.when(live)(put)
                else:
                    put()

    out = jax.ShapeDtypeStruct((2, rows.row_blocks * width, own_k * width), F32)
    return pl.pallas_call(
        kernel,
        name="place",
        in_specs=[SMEM, VMEM],
        out_specs=VMEM,
        out_shape=out,
        compiler_params=limits(out, sel),
    )(structure, sel)


def finish_band(k_inv, terms):
    def kernel(k_ref, *refs):
        *term_refs, out_ref = refs
        row = lax.axis_index("prow")
        band = out_ref.shape[2]
        total = term_refs[0][...].astype(F32)
        for ref in term_refs[1:]:
            total += ref[...].astype(F32)
        at = pl.ds(pl.multiple_of(row * band, band), band)
        out_ref[...] = (k_ref[:, :, at, :] - total).astype(BF16)

    return pl.pallas_call(
        kernel,
        name="finish_band",
        in_specs=[VMEM] * (1 + len(terms)),
        out_specs=VMEM,
        out_shape=jax.ShapeDtypeStruct(terms[0].shape, BF16),
        compiler_params=limits(k_inv, *terms),
    )(k_inv, *terms)


def join_bands(bands, shape):
    def kernel(*refs):
        *band_refs, out_ref = refs
        band = band_refs[0].shape[2]
        for k, ref in enumerate(band_refs):
            at = pl.ds(pl.multiple_of(member(-k) * band, band), band)
            out_ref[:, :, at, :] = ref[...].astype(F32)

    return pl.pallas_call(
        kernel,
        name="join_bands",
        in_specs=[VMEM] * len(bands),
        out_specs=VMEM,
        out_shape=jax.ShapeDtypeStruct(shape, F32),
        compiler_params=limits(jax.ShapeDtypeStruct(shape, F32), *bands),
    )(*bands)


def gather_rows(pieces):
    n = lax.axis_size("prow")
    held = [(0, tuple(dxs), value) for dxs, value in pieces]
    d = n // 2
    while d:
        here = [(at, dxs, swap(value, "prow", d)) for at, dxs, value in held if at == 0]
        for at in sorted({at for at, _, _ in held if at}):
            parts = [(dxs, value) for far, dxs, value in held if far == at]
            value = parts[0][1] if len(parts) == 1 else jnp.concatenate([value for _, value in parts])
            dxs = sum((dxs for dxs, _ in parts), ())
            here.append((at, dxs, swap(value, "prow", d)))
        held += [(at ^ d, dxs, value) for at, dxs, value in here]
        d //= 2
    return [(f"z{dxs[0]}{at}", value, at, dxs) for at, dxs, value in held]


def local(ainv_anc, panel, u_inv, k_inv, structure):
    width = u_inv.shape[-1]
    own_k = k_inv.shape[1]
    n_rows, n_cols = lax.axis_size("prow"), lax.axis_size("pcol")
    rows = Rows(ainv_anc.shape[1] // width, ainv_anc.shape[2] // width, structure.shape[1] // n_cols)
    near, far = list(range(n_cols // 2)), list(range(n_cols // 2, n_cols))
    sent, structure = pick_panel(panel, structure, own_k)
    got = [sent[0]] + [swap(sent[d], "pcol", d) for d in range(1, n_cols)]
    early, late = [], []
    pieces = [(dxs, jnp.stack([got[d] for d in dxs])) for dxs in (near, far)]
    last = f"z{far[0]}{n_rows - 1}"
    if n_rows > FEW:
        for dxs, value in pieces:
            (early if set(dxs) <= set(near) else late).append(([lax.all_gather(value, "prow")], None, dxs))
    else:
        for name, value, at, dxs in gather_rows(pieces[:1]) + gather_rows(pieces[1:]):
            (late if name == last else early).append(([value], [at], dxs))
    blocks = dict(zip(far, pick_ainv(ainv_anc, structure, own_k, width, rows, far), strict=True))
    blocks.update(zip(near, pick_ainv(ainv_anc, structure, own_k, width, rows, near), strict=True))
    ainv = [blocks[0]] + [swap(blocks[d], "pcol", d) for d in range(1, n_cols)]
    found = solve_early(structure, u_inv, early, near, ainv, rows)
    sel, terms = solve_late(structure, u_inv, late, found, far, ainv, rows)
    sel_inv = place(structure, sel, rows)
    if n_rows > FEW:
        total = lax.psum_scatter(terms[0], "prow", scatter_dimension=2, tiled=True)
        mine = finish_band(k_inv, [total])
        return sel_inv, lax.all_gather(mine, "prow", axis=2, tiled=True).astype(F32)
    terms = [terms[0]] + [turn(terms[k], k) for k in range(1, n_rows)]
    mine = finish_band(k_inv, terms)
    bands = [mine] + [turn(mine, k) for k in range(1, n_rows)]
    return sel_inv, join_bands(bands, k_inv.shape)


def solution(mesh):
    placed = (
        P(None, ("pole", "prow"), "pcol"),
        P(None, "pole", ("pcol", "prow"), None),
        P(None, "pole", None, None),
        P(None, ("pole", "pcol"), None, None),
        P(),
    )
    return jax.shard_map(
        local,
        mesh=mesh,
        in_specs=placed,
        out_specs=(P(None, ("pole", "prow"), "pcol"), P(None, ("pole", "pcol"), None, None)),
        check_vma=False,
    )
```
